64 devices in a mesh: rep: 4 (over x, y), dp: 16 (over z, core).
Axes of the slice: x: 2, y: 2, z: 8, core: 2. Of those that a mesh axis runs over, the one named last changes fastest.
The devices are a block of a 4x4x8 slice.
Arguments:
- x: bfloat16 [64, 2048, 768], P(('rep', 'dp')), parts along dimension 0
- dy: bfloat16 [64, 2048, 768], P(('rep', 'dp')), parts along dimension 0
- w_gate: bfloat16 [2, 768, 2304], replicated
- w_up: bfloat16 [2, 768, 2304], replicated
- w_down: bfloat16 [2, 2304, 768], replicated
- m_w_gate: float32 [2, 768, 2304], replicated
- m_w_up: float32 [2, 768, 2304], replicated
- m_w_down: float32 [2, 2304, 768], replicated
- v_w_gate: float32 [2, 768, 2304], replicated
- v_w_up: float32 [2, 768, 2304], replicated
- v_w_down: float32 [2, 2304, 768], replicated
Outputs:
- output 1: bfloat16 [8, 768, 2304], P('rep'), parts along dimension 0
- output 2: bfloat16 [8, 768, 2304], P('rep'), parts along dimension 0
- output 3: bfloat16 [8, 2304, 768], P('rep'), parts along dimension 0
- output 4: float32 [8, 768, 2304], P('rep'), parts along dimension 0
- output 5: float32 [8, 768, 2304], P('rep'), parts along dimension 0
- output 6: float32 [8, 2304, 768], P('rep'), parts along dimension 0
- output 7: float32 [8, 768, 2304], P('rep'), parts along dimension 0
- output 8: float32 [8, 768, 2304], P('rep'), parts along dimension 0
- output 9: float32 [8, 2304, 768], P('rep'), parts along dimension 0
There are 4 independent parts. The reference program is written for one: setup_inputs(seed, part) draws one part's arguments, and reference() takes and returns one part's arrays. A program takes and returns all parts, laid end to end along the dimension named above; an argument that names none is the same for every part.
All inputs are finite; a program needn't handle non-finite values.
Results may differ from the reference program's by a relative error of at most 0.0224.
Values are sent between devices in bfloat16 or wider.
A program may use at most 768 MiB of HBM per device.

```python
import jax
import jax.numpy as jnp
from jax import lax

SEQUENCES = 16
TOKENS = 2048
D = 768
FF = 2304
LAYERS = 2
NAMES = ("w_gate", "w_up", "w_down")
SHAPES = {"w_gate": (LAYERS, D, FF), "w_up": (LAYERS, D, FF), "w_down": (LAYERS, FF, D)}


def bump(key, n, height):
    away = (jnp.arange(n, dtype=jnp.int32) - jax.random.randint(key, (), 0, n, jnp.int32)) % n
    return jnp.where(away < n // 8, height, 1.0)


def together(key, own, strength):
    shared = jax.random.normal(key, own.shape[1:], jnp.float32)
    return (own + strength * shared) * lax.rsqrt(1 + strength * strength)


def setup_inputs(seed: int = 0, part: int = 0) -> dict:
    kx, kdy, ka, kb, kz, kf, kh, kl, *keys = jax.random.split(jax.random.key(seed), 8 + 3 * len(NAMES))
    kx, kdy, ka, kb = (jax.random.fold_in(k, part) for k in (kx, kdy, ka, kb))
    kw, km, kv = (keys[i::3] for i in range(3))
    shape = (SEQUENCES, TOKENS, D)
    much_x, much_dy = jax.random.uniform(kz, (2,), jnp.float32, 0.0, 1.0)
    loud = 2.0 ** jax.random.uniform(jax.random.fold_in(kz, 1), (), jnp.float32, -1.0, 2.0)
    layers = 2.0 ** jax.random.uniform(kl, (LAYERS, 1, 1), jnp.float32, -1.0, 1.0)
    x = together(ka, jax.random.normal(kx, shape, jnp.float32), much_x) * bump(kf, D, 4.0)
    dy = together(kb, jax.random.normal(kdy, shape, jnp.float32), much_dy)
    drawn = {"x": x.astype(jnp.bfloat16), "dy": (loud * dy * (SEQUENCES * TOKENS) ** -0.5).astype(jnp.bfloat16)}
    for key, name in zip(kw, NAMES, strict=True):
        w = jax.random.normal(key, SHAPES[name], jnp.float32) * SHAPES[name][1] ** -0.5
        drawn[name] = (w * {"w_gate": 1.0, "w_up": bump(kh, FF, 4.0), "w_down": layers}[name]).astype(jnp.bfloat16)
    for key, name in zip(km, NAMES, strict=True):
        drawn[f"m_{name}"] = 0.1 * jax.random.normal(key, SHAPES[name], jnp.float32)
    for key, name in zip(kv, NAMES, strict=True):
        drawn[f"v_{name}"] = jax.random.uniform(key, SHAPES[name], jnp.float32, 0.005, 0.015)
    return drawn


def matmul(a, w):
    return jnp.dot(a, w, preferred_element_type=jnp.float32).astype(jnp.bfloat16)


def normed(h):
    wide = h.astype(jnp.float32)
    scale = lax.rsqrt(jnp.mean(wide**2, -1, keepdims=True) + 1e-6)
    return (wide * scale).astype(jnp.bfloat16)


def layer(h, w):
    a = normed(h)
    gate = jnp.dot(a, w["w_gate"], preferred_element_type=jnp.float32)
    up = jnp.dot(a, w["w_up"], preferred_element_type=jnp.float32)
    return h + matmul((jax.nn.silu(gate) * up).astype(jnp.bfloat16), w["w_down"])


def adamw(w, m, v, g):
    m = 0.9 * m + 0.1 * g
    v = 0.95 * v + 0.05 * g * g
    step = m * lax.rsqrt(v + 1e-8) + 0.1 * w
    return (w - 0.02 * step).astype(jnp.bfloat16), m, v


def clipped(gradients, sum_of_squares, count):
    factor = jnp.minimum(1.0, 0.5 * lax.rsqrt(sum_of_squares / count + 1e-30))
    return [g * factor for g in gradients]


def stack(weights, h):
    return lax.scan(lambda h, w: (layer(h, w), None), h, weights)[0]


def reference(x, dy, w_gate, w_up, w_down, m_w_gate, m_w_up, m_w_down, v_w_gate, v_w_up, v_w_down):
    weights = dict(zip(NAMES, (w_gate, w_up, w_down), strict=True))

    def take(so_far, sequence):
        h, by_y = sequence
        _, back = jax.vjp(lambda w: stack(w, h), weights)
        return jax.tree.map(lambda total, term: total + term.astype(jnp.float32), so_far, back(by_y)[0]), None

    none_yet = {name: jnp.zeros(w.shape, jnp.float32) for name, w in weights.items()}
    by_weights, _ = lax.scan(take, none_yet, (x, dy))
    gradients = [by_weights[name].astype(jnp.bfloat16).astype(jnp.float32) for name in NAMES]
    gradients = clipped(gradients, sum(jnp.sum(g * g) for g in gradients), sum(g.size for g in gradients))
    new = [
        adamw(w.astype(jnp.float32), m, v, g)
        for w, m, v, g in zip((w_gate, w_up, w_down), (m_w_gate, m_w_up, m_w_down), (v_w_gate, v_w_up, v_w_down), gradients, strict=True)
    ]
    return tuple(one[which] for which in range(3) for one in new)
```

```python
import functools

import jax
import jax.numpy as jnp
from jax import lax
from jax.experimental import pallas as pl
from jax.experimental.pallas import tpu as pltpu
from jax.sharding import PartitionSpec as P

MESH = pl.DeviceIdType.MESH
F32, BF16 = jnp.float32, jnp.bfloat16
EVERY = pl.BlockSpec(memory_space=pl.ANY)
VMEM = pl.BlockSpec(memory_space=pltpu.VMEM)


def rounded(a, b, contract=((1,), (0,))):
    return lax.dot_general(a, b, (contract, ((), ())), preferred_element_type=F32).astype(BF16)


def wide_dot(a, b):
    return jnp.dot(a, b, preferred_element_type=F32)


def scale_of(wide):
    return lax.rsqrt(jnp.mean(wide * wide, -1, keepdims=True) + 1e-6)


def normed(h):
    wide = h.astype(F32)
    return (wide * scale_of(wide)).astype(BF16)


def gated(gate, up):
    return (gate * jax.nn.sigmoid(gate) * up).astype(BF16)


def gated_back(gate, up, by_mid):
    by_mid = by_mid.astype(F32)
    one = jax.nn.sigmoid(gate)
    silu = gate * one
    by_gate = by_mid * up * (one * (1.0 + gate * (1.0 - one)))
    return (silu * up).astype(BF16), by_gate.astype(BF16), (by_mid * silu).astype(BF16)


def params(mib, **more):
    return pltpu.CompilerParams(vmem_limit_bytes=mib << 20, **more)


def cost(matmuls, tokens, d, ff, moved):
    return pl.CostEstimate(flops=2 * matmuls * tokens * d * ff, bytes_accessed=moved, transcendentals=tokens * ff)


def up_kernel(h_ref, gate_ref, up_ref, a_ref, mid_ref):
    @pl.when(pl.program_id(1) == 0)
    def _():
        a_ref[...] = normed(h_ref[...])

    a = a_ref[...]
    mid_ref[...] = gated(wide_dot(a, gate_ref[0]), wide_dot(a, up_ref[0]))


def columns_of(number, d, block):
    return pl.BlockSpec((1, d, block), lambda i, k: (number, 0, k))


def rows_of(number, d, block):
    return pl.BlockSpec((1, block, d), lambda i, k: (number, k, 0))


def forward_up(number, h, w_gate, w_up, tall=1024, block=768):
    tokens, d = h.shape
    ff = w_gate.shape[2]
    rows = pl.BlockSpec((tall, d), lambda i, k: (i, 0))
    part = pl.BlockSpec((tall, block), lambda i, k: (i, k))
    return pl.pallas_call(
        up_kernel,
        out_shape=(jax.ShapeDtypeStruct((tokens, d), BF16), jax.ShapeDtypeStruct((tokens, ff), BF16)),
        grid=(tokens // tall, ff // block),
        in_specs=[rows, columns_of(number, d, block), columns_of(number, d, block)],
        out_specs=(rows, part),
        compiler_params=params(50),
        cost_estimate=cost(2, tokens, d, ff, 26 << 20),
        name="forward_up",
    )(h, w_gate, w_up)


def down_kernel(mid_ref, down_ref, h_ref, out_ref):
    out_ref[...] = h_ref[...] + rounded(mid_ref[...], down_ref[0])


def forward_down(number, mid, w_down, h, tall=512):
    tokens, d = h.shape
    ff = mid.shape[1]
    rows = pl.BlockSpec((tall, d), lambda i: (i, 0))
    return pl.pallas_call(
        down_kernel,
        out_shape=jax.ShapeDtypeStruct((tokens, d), BF16),
        grid=(tokens // tall,),
        in_specs=[pl.BlockSpec((tall, ff), lambda i: (i, 0)), pl.BlockSpec((1, ff, d), lambda i: (number, 0, 0)), rows],
        out_specs=rows,
        compiler_params=params(50),
        cost_estimate=cost(1, tokens, d, ff, 20 << 20),
        name="forward_down",
    )(mid, w_down, h)


def last_kernel(h_ref, by_ref, gate_ref, up_ref, down_ref, a_ref, mid_ref, by_gate_ref, by_up_ref):
    @pl.when(pl.program_id(1) == 0)
    def _():
        a_ref[...] = normed(h_ref[...])

    a = a_ref[...]
    by_mid = rounded(by_ref[...], down_ref[0], ((1,), (1,)))
    mid_ref[...], by_gate_ref[...], by_up_ref[...] = gated_back(wide_dot(a, gate_ref[0]), wide_dot(a, up_ref[0]), by_mid)


def last_layer(number, h, by, w_gate, w_up, w_down, tall=1024, block=768):
    tokens, d = h.shape
    ff = w_gate.shape[2]
    rows = pl.BlockSpec((tall, d), lambda i, k: (i, 0))
    part = pl.BlockSpec((tall, block), lambda i, k: (i, k))
    return pl.pallas_call(
        last_kernel,
        out_shape=(jax.ShapeDtypeStruct((tokens, d), BF16),) + (jax.ShapeDtypeStruct((tokens, ff), BF16),) * 3,
        grid=(tokens // tall, ff // block),
        in_specs=[rows, rows, columns_of(number, d, block), columns_of(number, d, block), rows_of(number, d, block)],
        out_specs=(rows, part, part, part),
        compiler_params=params(60),
        cost_estimate=cost(3, tokens, d, ff, 60 << 20),
        name="last_layer",
    )(h, by, w_gate, w_up, w_down)


def weight_kernel(a_ref, by_ref, mid_ref, by_gate_ref, by_up_ref, gate_ref, up_ref, down_ref, turned):
    @pl.when(pl.program_id(0) == 0)
    def _():
        turned[...] = a_ref[...].T

    gate_ref[...] = rounded(turned[...], by_gate_ref[...])
    up_ref[...] = rounded(turned[...], by_up_ref[...])
    down_ref[...] = rounded(mid_ref[...], by_ref[...], ((0,), (0,)))


def by_weights(a, by, mid, by_gate, by_up, block=768):
    tokens, d = a.shape
    ff = mid.shape[1]
    whole = pl.BlockSpec((tokens, d), lambda k: (0, 0), pipeline_mode=pl.Buffered(1))
    part = pl.BlockSpec((tokens, block), lambda k: (0, k))
    out = pl.BlockSpec((d, block), lambda k: (0, k))
    return pl.pallas_call(
        weight_kernel,
        out_shape=(jax.ShapeDtypeStruct((d, ff), BF16),) * 2 + (jax.ShapeDtypeStruct((ff, d), BF16),),
        grid=(ff // block,),
        in_specs=[whole, whole, part, part, part],
        out_specs=(out, out, pl.BlockSpec((block, d), lambda k: (k, 0))),
        scratch_shapes=[pltpu.VMEM((d, tokens), BF16)],
        compiler_params=params(56),
        cost_estimate=cost(3, tokens, d, ff, 45 << 20),
        name="by_weights",
    )(a, by, mid, by_gate, by_up)


class Ring:
    def __init__(self, n, grads, refs):
        self.n, self.chips, self.grads = n, n // 2, grads
        self.wide_own, self.wide_pair, self.wide_ring, self.tall_own, self.tall_pair, self.tall_ring = refs[:6]
        self.local, self.pair_send, self.pair_recv, self.ring_send, self.ring_recv = refs[6:]
        self.me = lax.axis_index("dp")
        self.z, self.c = self.me // 2, lax.rem(self.me, 2)
        self.partner = self.z * 2 + 1 - self.c
        self.beside = [lax.rem(self.z + k, self.chips) * 2 + self.c for k in (1, self.chips - 1)]

    @staticmethod
    def scratch(n, wide, tall):
        chips, sem = n // 2, pltpu.SemaphoreType.DMA
        return [
            pltpu.VMEM((2, chips, *wide), BF16),
            pltpu.VMEM((2, chips, *wide), BF16),
            pltpu.VMEM((2, chips - 1, *wide), BF16),
            pltpu.VMEM((chips, *tall), BF16),
            pltpu.VMEM((chips, *tall), BF16),
            pltpu.VMEM((chips - 1, *tall), BF16),
            sem((3, chips)), sem((3, chips)), sem((3, chips)), sem((3, 2, chips - 1)), sem((3, 2, chips - 1)),
        ]

    def chunk(self, way, step):
        return lax.rem(self.z + self.chips + ((-1 - step) if way == 0 else (1 + step - self.chips)), self.chips)

    def refs(self, i, j):
        if i < 2:
            return self.wide_own.at[i, j], self.wide_pair.at[i, j], lambda step: self.wide_ring.at[i, step]
        return self.tall_own.at[j], self.tall_pair.at[j], lambda step: self.tall_ring.at[step]

    def exchange(self, i, j):
        own, pair, _ = self.refs(i, j)
        return (
            pltpu.make_async_copy(self.grads[i].at[j, self.c], own, self.local.at[i, j]),
            pltpu.make_async_remote_copy(
                src_ref=self.grads[i].at[j, 1 - self.c], dst_ref=pair, send_sem=self.pair_send.at[i, j], recv_sem=self.pair_recv.at[i, j],
                device_id={"dp": self.partner}, device_id_type=MESH,
            ),
        )

    def greet(self, everyone):
        barrier = pltpu.get_barrier_semaphore()
        others = [lax.rem(self.me + k, self.n) for k in range(1, self.n)] if everyone else [self.partner, *self.beside]
        for other in others:
            pl.semaphore_signal(barrier, inc=1, device_id={"dp": other}, device_id_type=MESH)
        pl.semaphore_wait(barrier, len(others))

    def new_chunks(self, step):
        half = self.chips // 2
        if step < half - 1:
            return [self.chunk(0, step), self.chunk(1, step)]
        return [self.chunk(0, step)] if step in (half - 1, self.chips - 1) else []

    def begin(self):
        for step in range(self.chips):
            for j in self.new_chunks(step):
                for i in range(3):
                    for copy in self.exchange(i, j):
                        copy.start()

    def half(self, i, way):
        columns = self.grads[i].shape[3] // 2
        return slice(None), slice(columns * way, columns * (way + 1))

    def hop(self, i, way, step):
        own, _, ring = self.refs(i, self.chunk(way, step))
        at = self.half(i, way)
        return pltpu.make_async_remote_copy(
            src_ref=own.at[at], dst_ref=ring(step).at[at], send_sem=self.ring_send.at[i, way, step], recv_sem=self.ring_recv.at[i, way, step],
            device_id={"dp": self.beside[way]}, device_id_type=MESH,
        )

    def ready(self, i, step):
        for j in self.new_chunks(step):
            for copy in self.exchange(i, j):
                copy.wait()

    def total(self, i, j, at, step):
        own, pair, ring = self.refs(i, j)
        value = own[at].astype(F32) + pair[at].astype(F32)
        if step:
            value = value + ring(step - 1)[at].astype(F32)
        return value.astype(BF16)

    def send(self, step):
        for i in range(3):
            self.ready(i, step)
            for way in range(2):
                if step:
                    self.hop(i, way, step - 1).wait_recv()
                j, at = self.chunk(way, step), self.half(i, way)
                self.refs(i, j)[0][at] = self.total(i, j, at, step)
            for way in range(2):
                self.hop(i, way, step).start()

    def finish(self, out):
        last = self.chips - 1
        for i in range(3):
            self.ready(i, last)
            for way in range(2):
                self.hop(i, way, last - 1).wait_recv()
            value = self.total(i, self.z, (slice(None), slice(None)), last)
            rows, columns = out.shape[1], value.shape[1]
            for k in range(value.shape[0] // rows):
                out[i, :, columns * k : columns * (k + 1)] = value[rows * k : rows * (k + 1)]
        for i in range(3):
            for way in range(2):
                for step in range(last):
                    self.hop(i, way, step).wait_send()


def squares_of(ref):
    squares = jnp.zeros((8, 128), F32)
    for i in range(ref.shape[0]):
        value = ref[i].astype(F32)
        flat = jnp.sum((value * value).reshape(-1, 8, value.shape[1]), axis=0)
        for k in range(flat.shape[1] // 128):
            squares = squares + flat[:, 128 * k : 128 * (k + 1)]
    return squares


def ring_kernel(n, *refs):
    grads, before_ref, out_ref, ss_ref, parts, ss_send, ss_recv = refs[:3], *refs[3:9]
    ring = Ring(n, grads, refs[9:])
    ring.greet(True)
    ring.begin()
    for step in range(ring.chips - 1):
        ring.send(step)
    me = ring.me
    before = squares_of(before_ref)
    ring.finish(out_ref)
    parts[me] = before + squares_of(out_ref)

    def tell(k):
        return pltpu.make_async_remote_copy(
            src_ref=parts.at[me], dst_ref=parts.at[me], send_sem=ss_send.at[k], recv_sem=ss_recv.at[k],
            device_id={"dp": lax.rem(me + k, n)}, device_id_type=MESH,
        )

    for k in range(1, n):
        tell(k).start()
    for k in range(1, n):
        tell(k).wait()
    everyone = parts[0]
    for k in range(1, n):
        everyone = everyone + parts[k]
    ss_ref[...] = everyone


def chunked(n, grads):
    return [g.reshape(n // 2, 2, g.shape[0] // n, g.shape[1]) for g in grads]


def summed(n, grads, before):
    shaped = chunked(n, grads)
    wide, tall = shaped[0].shape[2:], shaped[2].shape[2:]
    return pl.pallas_call(
        functools.partial(ring_kernel, n),
        out_shape=(jax.ShapeDtypeStruct((3, *wide), BF16), jax.ShapeDtypeStruct((8, 128), F32)),
        in_specs=[EVERY] * 3 + [VMEM],
        out_specs=(VMEM,) * 2,
        scratch_shapes=[pltpu.VMEM((n, 8, 128), F32), pltpu.SemaphoreType.DMA((n,)), pltpu.SemaphoreType.DMA((n,)), *Ring.scratch(n, wide, tall)],
        compiler_params=params(40, collective_id=0, has_side_effects=True),
        name="ring_sum",
    )(*shaped, before)


def first_kernel(n, block, *refs):
    grads = refs[:3]
    by_gate1, by_up1, gate1, up1, h1, by1, gate0, up0, down0, a0 = refs[3:13]
    out_ref, by_ref, by_gate_ref, by_up_ref = refs[13:17]
    ring = Ring(n, grads, refs[17:])
    tile = pl.program_id(0)
    tiles = (ring.chips - 1 + 1) // 2

    @pl.when(tile == 0)
    def _():
        ring.greet(False)
        ring.begin()

    def moment(which):
        for k in range(tiles):
            step = 2 * k + which

            @pl.when(tile == k)
            def _():
                if step < ring.chips - 1:
                    ring.send(step)
                else:
                    ring.finish(out_ref)

    last = ((1,), (1,))
    by_a = rounded(by_gate1[...], gate1[0], last) + rounded(by_up1[...], up1[0], last)
    wide, by_a = h1[...].astype(F32), by_a.astype(F32)
    scale = scale_of(wide)
    dots = jnp.sum(by_a * wide, -1, keepdims=True) / wide.shape[1]
    by_ref[...] = by1[...] + (by_a * scale - wide * (scale * scale * scale * dots)).astype(BF16)
    moment(0)
    by, a = by_ref[...], a0[...]
    for k in range(gate0.shape[2] // block):
        at = slice(block * k, block * (k + 1))
        by_mid = rounded(by, down0[0, at, :], last)
        _, by_gate_ref[:, at], by_up_ref[:, at] = gated_back(wide_dot(a, gate0[0, :, at]), wide_dot(a, up0[0, :, at]), by_mid)
    moment(1)


def first_layer(n, grads, by_gate, by_up, h, by, a, w_gate, w_up, w_down, block=768):
    shaped = chunked(n, grads)
    wide, tall = shaped[0].shape[2:], shaped[2].shape[2:]
    tokens, d = h.shape
    ff = by_gate.shape[1]
    deep = tokens // (n // 4)

    def whole(number, w):
        return pl.BlockSpec((1, *w.shape[1:]), lambda i: (number, 0, 0), pipeline_mode=pl.Buffered(1))

    rows, long = pl.BlockSpec((deep, d), lambda i: (i, 0)), pl.BlockSpec((deep, ff), lambda i: (i, 0))
    return pl.pallas_call(
        functools.partial(first_kernel, n, block),
        out_shape=(
            jax.ShapeDtypeStruct((3, *wide), BF16),
            jax.ShapeDtypeStruct((tokens, d), BF16),
            jax.ShapeDtypeStruct((tokens, ff), BF16),
            jax.ShapeDtypeStruct((tokens, ff), BF16),
        ),
        grid=(n // 4,),
        in_specs=[EVERY] * 3 + [long, long, whole(1, w_gate), whole(1, w_up), rows, rows, whole(0, w_gate), whole(0, w_up), whole(0, w_down), rows],
        out_specs=(pl.BlockSpec((3, *wide), lambda i: (0, 0, 0)), rows, long, long),
        scratch_shapes=Ring.scratch(n, wide, tall),
        compiler_params=params(60, collective_id=1, has_side_effects=True, dimension_semantics=("arbitrary",)),
        cost_estimate=cost(5, tokens, d, ff, 60 << 20),
        name="first_layer",
    )(*shaped, by_gate, by_up, w_gate, w_up, h, by, w_gate, w_up, w_down, a)


def adam_kernel(first, where_ref, factor_ref, *refs):
    pieces, (w, m, v) = refs[:4], (refs[4:7], refs[7:10], refs[10:13])
    new_w, new_m, new_v = (refs[i : i + 3] for i in ((13, 16, 19) if first else (22, 25, 28)))
    g_ref = refs[-1]
    part = pl.program_id(0)
    for p in range(4):

        @pl.when(part == p)
        def _():
            g_ref[...] = pieces[p][...]

    factor = factor_ref[0]
    for which in range(3):
        rows, columns = w[which].shape[1:]
        deep = g_ref.shape[1]
        for k in range(rows // deep):
            at = (0, slice(deep * k, deep * (k + 1)), slice(None))
            g = g_ref[which, :, columns * k : columns * (k + 1)].astype(F32) * factor
            mean = 0.9 * m[which][at] + 0.1 * g
            square = 0.95 * v[which][at] + 0.05 * g * g
            wide = w[which][at].astype(F32)
            new_m[which][at] = mean
            new_v[which][at] = square
            new_w[which][at] = (wide - 0.02 * (mean * lax.rsqrt(square + 1e-8) + 0.1 * wide)).astype(BF16)


def adam(n, where, factor, pieces, state, so_far):
    first = so_far is None
    shapes = [jax.ShapeDtypeStruct(s.shape, s.dtype) for s in state]

    def block(s):
        return pl.BlockSpec((1, s.shape[1] // n, s.shape[2]), lambda p, where, factor: (where[0, p], where[1, p], 0))

    whole = pl.BlockSpec(pieces[0].shape, lambda p, where, factor: (0, 0, 0))
    size = sum(s.size // n for s in state[:3]) * 4
    return pl.pallas_call(
        functools.partial(adam_kernel, first),
        out_shape=shapes,
        grid_spec=pltpu.PrefetchScalarGridSpec(
            num_scalar_prefetch=2,
            grid=(4,),
            in_specs=[whole] * 4 + [block(s) for s in state] + ([] if first else [EVERY] * 9),
            out_specs=[block(s) for s in state],
            scratch_shapes=[pltpu.VMEM(pieces[0].shape, BF16)],
        ),
        input_output_aliases={} if first else {15 + i: i for i in range(9)},
        compiler_params=pltpu.CompilerParams(vmem_limit_bytes=40 << 20, dimension_semantics=("arbitrary",)),
        cost_estimate=pl.CostEstimate(flops=60_000_000, bytes_accessed=size * 11, transcendentals=size // 4),
        name="adam_step",
    )(where, factor, *pieces, *state, *(so_far or ()))


def solution(mesh):
    n = mesh.shape["dp"]
    chips = n // 2

    def step(x, dy, *arrays):
        weights, m, v = (arrays[i : i + 3] for i in (0, 3, 6))
        w_gate, w_up, w_down = weights
        x, dy = x[0], dy[0]
        a0, mid0 = forward_up(0, x, w_gate, w_up)
        h1 = forward_down(0, mid0, w_down, x)
        a1, mid1, by_gate1, by_up1 = last_layer(1, h1, dy, w_gate, w_up, w_down)
        grads1 = by_weights(a1, dy, mid1, by_gate1, by_up1)
        right, by, by_gate0, by_up0 = first_layer(n, grads1, by_gate1, by_up1, h1, dy, a0, w_gate, w_up, w_down)
        grads0 = by_weights(a0, by, mid0, by_gate0, by_up0)
        left, squares = summed(n, grads0, right)
        count = sum(w.size for w in weights)
        factor = jnp.minimum(1.0, 0.5 * lax.rsqrt(jnp.sum(squares) / count + 1e-30)).reshape(1)

        me = lax.axis_index("dp")
        z, c = me // 2, me % 2
        ahead = [(i, (i + 2) % n) for i in range(n)]
        behind = [(i, (i + n - 2) % n) for i in range(n)]
        pairs = [(i, i ^ 1) for i in range(n)]
        new = None
        for hop in range(chips):
            if hop:
                right = lax.ppermute(right, "dp", ahead)
                left = lax.ppermute(left, "dp", behind)
            pieces = [right, lax.ppermute(right, "dp", pairs), left, lax.ppermute(left, "dp", pairs)]
            from_right, from_left = (z + chips - hop) % chips * 2, (z + hop) % chips * 2
            where = jnp.array([[1, 1, 0, 0], [0, 0, 0, 0]], jnp.int32).at[1].set(
                jnp.stack([from_right + c, from_right + 1 - c, from_left + c, from_left + 1 - c])
            )
            new = adam(n, where, factor, pieces, (*weights, *m, *v), new)
        return tuple(new)

    return jax.shard_map(
        step,
        mesh=mesh,
        in_specs=(P(("rep", "dp"), None, None),) * 2 + (P(None, None, None),) * 9,
        out_specs=(P("rep", None, None),) * 9,
        check_vma=False,
    )
```

```python
import functools

import jax
import jax.numpy as jnp
from jax import lax
from jax.experimental import pallas as pl
from jax.experimental.pallas import tpu as pltpu
from jax.sharding import PartitionSpec as P

MESH = pl.DeviceIdType.MESH
F32, BF16 = jnp.float32, jnp.bfloat16
EVERY = pl.BlockSpec(memory_space=pl.ANY)
VMEM = pl.BlockSpec(memory_space=pltpu.VMEM)


def rounded(a, b, contract=((1,), (0,))):
    return lax.dot_general(a, b, (contract, ((), ())), preferred_element_type=F32).astype(BF16)


def wide_dot(a, b):
    return jnp.dot(a, b, preferred_element_type=F32)


def scale_of(wide):
    return lax.rsqrt(jnp.mean(wide * wide, -1, keepdims=True) + 1e-6)


def normed(h):
    wide = h.astype(F32)
    return (wide * scale_of(wide)).astype(BF16)


def gated(gate, up):
    return (gate * jax.nn.sigmoid(gate) * up).astype(BF16)


def gated_back(gate, up, by_mid):
    by_mid = by_mid.astype(F32)
    one = jax.nn.sigmoid(gate)
    silu = gate * one
    by_gate = by_mid * up * (one * (1.0 + gate * (1.0 - one)))
    return (silu * up).astype(BF16), by_gate.astype(BF16), (by_mid * silu).astype(BF16)


def params(mib, **more):
    return pltpu.CompilerParams(vmem_limit_bytes=mib << 20, **more)


def cost(matmuls, tokens, d, ff, moved):
    return pl.CostEstimate(flops=2 * matmuls * tokens * d * ff, bytes_accessed=moved, transcendentals=tokens * ff)


def up_kernel(h_ref, gate_ref, up_ref, a_ref, mid_ref):
    @pl.when(pl.program_id(1) == 0)
    def _():
        a_ref[...] = normed(h_ref[...])

    a = a_ref[...]
    mid_ref[...] = gated(wide_dot(a, gate_ref[0]), wide_dot(a, up_ref[0]))


def columns_of(number, d, block):
    return pl.BlockSpec((1, d, block), lambda i, k: (number, 0, k))


def rows_of(number, d, block):
    return pl.BlockSpec((1, block, d), lambda i, k: (number, k, 0))


def forward_up(number, h, w_gate, w_up, tall=1024, block=768):
    tokens, d = h.shape
    ff = w_gate.shape[2]
    rows = pl.BlockSpec((tall, d), lambda i, k: (i, 0))
    part = pl.BlockSpec((tall, block), lambda i, k: (i, k))
    return pl.pallas_call(
        up_kernel,
        out_shape=(jax.ShapeDtypeStruct((tokens, d), BF16), jax.ShapeDtypeStruct((tokens, ff), BF16)),
        grid=(tokens // tall, ff // block),
        in_specs=[rows, columns_of(number, d, block), columns_of(number, d, block)],
        out_specs=(rows, part),
        compiler_params=params(63),
        cost_estimate=cost(2, tokens, d, ff, 26 << 20),
        name="forward_up",
    )(h, w_gate, w_up)


def down_kernel(mid_ref, down_ref, h_ref, out_ref):
    out_ref[...] = h_ref[...] + rounded(mid_ref[...], down_ref[0])


def forward_down(number, mid, w_down, h, tall=512):
    tokens, d = h.shape
    ff = mid.shape[1]
    rows = pl.BlockSpec((tall, d), lambda i: (i, 0))
    return pl.pallas_call(
        down_kernel,
        out_shape=jax.ShapeDtypeStruct((tokens, d), BF16),
        grid=(tokens // tall,),
        in_specs=[pl.BlockSpec((tall, ff), lambda i: (i, 0)), pl.BlockSpec((1, ff, d), lambda i: (number, 0, 0)), rows],
        out_specs=rows,
        compiler_params=params(63),
        cost_estimate=cost(1, tokens, d, ff, 20 << 20),
        name="forward_down",
    )(mid, w_down, h)


def last_kernel(h_ref, by_ref, gate_ref, up_ref, down_ref, a_ref, all_ref):
    @pl.when(pl.program_id(1) == 0)
    def _():
        a_ref[...] = normed(h_ref[...])

    a = a_ref[...]
    by_mid = rounded(by_ref[...], down_ref[0], ((1,), (1,)))
    all_ref[2], all_ref[0], all_ref[1] = gated_back(wide_dot(a, gate_ref[0]), wide_dot(a, up_ref[0]), by_mid)


def last_layer(number, h, by, w_gate, w_up, w_down, tall=1024, block=768):
    tokens, d = h.shape
    ff = w_gate.shape[2]
    rows = pl.BlockSpec((tall, d), lambda i, k: (i, 0))
    return pl.pallas_call(
        last_kernel,
        out_shape=(
            jax.ShapeDtypeStruct((tokens, d), BF16),
            jax.ShapeDtypeStruct((3, tokens, ff), BF16),
        ),
        grid=(tokens // tall, ff // block),
        in_specs=[rows, rows, columns_of(number, d, block), columns_of(number, d, block), rows_of(number, d, block)],
        out_specs=(rows, pl.BlockSpec((3, tall, block), lambda i, k: (0, i, k))),
        compiler_params=params(63),
        cost_estimate=cost(3, tokens, d, ff, 60 << 20),
        name="last_layer",
    )(h, by, w_gate, w_up, w_down)


def turn(a_ref, by_ref, turned):
    turned[0] = a_ref[...].T
    turned[1] = by_ref[...].T


def part_specs(tokens, d, ff, block):
    count = ff // block
    whole = pl.BlockSpec((tokens, d), lambda k: (0, 0), pipeline_mode=pl.Buffered(1))
    mid = pl.BlockSpec((tokens, block), lambda k: (0, jnp.minimum(k, count - 1)))
    both = pl.BlockSpec((1, tokens, block), lambda k: (jnp.maximum(k - count, 0) // count, 0, jnp.maximum(k - count, 0) % count))
    return [whole, whole, mid, both]


def weight_kernel(a_ref, by_ref, all_ref, wide_ref, down_ref, turned):
    now = pl.program_id(0)
    tall = now < pl.num_programs(0) // 3

    @pl.when(now == 0)
    def _():
        turn(a_ref, by_ref, turned)

    value = rounded(turned[jnp.where(tall, 1, 0)], all_ref[0])

    @pl.when(tall)
    def _():
        down_ref[...] = value.T

    @pl.when(jnp.logical_not(tall))
    def _():
        wide_ref[0] = value


def by_weights(a, by, every, block=768):
    tokens, d = a.shape
    ff = every.shape[2]
    count = ff // block
    whole, _, _, both = part_specs(tokens, d, ff, block)
    stacked = pl.BlockSpec((1, tokens, block), lambda k: (jnp.where(k < count, 2, k // count - 1), 0, k % count))
    return pl.pallas_call(
        weight_kernel,
        out_shape=(jax.ShapeDtypeStruct((2, d, ff), BF16), jax.ShapeDtypeStruct((ff, d), BF16)),
        grid=(3 * count,),
        in_specs=[whole, whole, stacked],
        out_specs=(pl.BlockSpec((1, d, block), both.index_map), pl.BlockSpec((block, d), lambda k: (jnp.minimum(k, count - 1), 0))),
        scratch_shapes=[pltpu.VMEM((2, d, tokens), BF16)],
        compiler_params=params(63, dimension_semantics=("arbitrary",)),
        cost_estimate=cost(3, tokens, d, ff, 45 << 20),
        name="by_weights",
    )(a, by, every)


def when(condition):
    if isinstance(condition, bool):
        return (lambda body: body()) if condition else (lambda body: None)
    return pl.when(condition)


class Ring:
    def __init__(self, n, grads, refs):
        self.n, self.chips, self.grads = n, n // 2, grads
        self.wide_own, self.wide_pair, self.wide_ring, self.tall_own, self.tall_pair, self.tall_ring = refs[:6]
        self.local, self.pair_send, self.pair_recv, self.ring_send, self.ring_recv = refs[6:]
        self.me = lax.axis_index("dp")
        self.z, self.c = self.me // 2, lax.rem(self.me, 2)
        self.partner = self.z * 2 + 1 - self.c
        self.beside = [lax.rem(self.z + k, self.chips) * 2 + self.c for k in (1, self.chips - 1)]

    @staticmethod
    def scratch(n, wide, tall, all_own):
        chips, sem = n // 2, pltpu.SemaphoreType.DMA
        own = n if all_own else chips
        bands = tall[0]
        return [
            pltpu.VMEM((2, own, *wide), BF16),
            pltpu.VMEM((2, chips, *wide), BF16),
            pltpu.VMEM((2, chips - 1, *wide), BF16),
            pltpu.VMEM((own * bands, *tall[1:]), BF16),
            pltpu.VMEM((chips * bands, *tall[1:]), BF16),
            pltpu.VMEM(((chips - 1) * bands, *tall[1:]), BF16),
            sem((3, chips)), sem((3, chips)), sem((3, chips)), sem((3, 2, chips - 1)), sem((3, 2, chips - 1)),
        ]

    def chunk(self, way, step):
        return lax.rem(self.z + (self.chips - 1 - step if way == 0 else 1 + step), self.chips)

    def at(self, i, wide, tall, j):
        if i < 2:
            return wide.at[i, j]
        bands = self.tall_ring.shape[0] // (self.chips - 1)
        return tall.at[pl.ds(j * bands, bands)]

    def own(self, i, j, theirs=False):
        if self.grads is None:
            j = 2 * j + (1 - self.c if theirs else self.c)
        return self.at(i, self.wide_own, self.tall_own, j)

    def pair(self, i, j):
        return self.at(i, self.wide_pair, self.tall_pair, j)

    def arriving(self, i, step):
        return self.at(i, self.wide_ring, self.tall_ring, step)

    def exchange(self, i, j):
        theirs = self.own(i, j, True) if self.grads is None else self.grads[i].at[j, 1 - self.c]
        away = pltpu.make_async_remote_copy(
            src_ref=theirs, dst_ref=self.pair(i, j), send_sem=self.pair_send.at[i, j], recv_sem=self.pair_recv.at[i, j],
            device_id={"dp": self.partner}, device_id_type=MESH,
        )
        if self.grads is None:
            return [away]
        return [away, pltpu.make_async_copy(self.grads[i].at[j, self.c], self.own(i, j), self.local.at[i, j])]

    def greet(self, everyone):
        barrier = pltpu.get_barrier_semaphore()
        others = [lax.rem(self.me + k, self.n) for k in range(1, self.n)] if everyone else [self.partner, *self.beside]
        for other in others:
            pl.semaphore_signal(barrier, inc=1, device_id={"dp": other}, device_id_type=MESH)
        pl.semaphore_wait(barrier, len(others))

    def begin(self, matrices):
        half = self.chips // 2
        for step in range(half):
            for way in range(2 if step < half - 1 else 1):
                for i in matrices:
                    for copy in self.exchange(i, self.chunk(way, step)):
                        copy.start()
        for i in matrices:
            for copy in self.exchange(i, self.z):
                copy.start()

    def ready(self, i, step):
        half = self.chips // 2

        @when(step < half)
        def _():
            for copy in self.exchange(i, self.chunk(0, step)):
                copy.wait()

        @when(step < half - 1)
        def _():
            for copy in self.exchange(i, self.chunk(1, step)):
                copy.wait()

    def half(self, i, way):
        columns = self.pair(i, 0).shape[-1] // 2
        return (slice(None),) * (1 if i < 2 else 2) + (slice(columns * way, columns * (way + 1)),)

    def hop(self, i, way, step):
        at = self.half(i, way)
        return pltpu.make_async_remote_copy(
            src_ref=self.own(i, self.chunk(way, step)).at[at], dst_ref=self.arriving(i, step).at[at],
            send_sem=self.ring_send.at[i, way, step], recv_sem=self.ring_recv.at[i, way, step],
            device_id={"dp": self.beside[way]}, device_id_type=MESH,
        )

    def add(self, i, way, j, step):
        own, pair, columns = self.own(i, j), self.pair(i, j), self.half(i, way)[-1]
        ring = None if step is None else self.arriving(i, step - 1)

        @pl.loop(0, 3)
        def _(part):
            deep = own.shape[0] // 3
            at = (pl.ds(pl.multiple_of(part * deep, deep), deep), columns) if i < 2 else (pl.ds(part * deep, deep), slice(None), columns)
            value = own[at].astype(F32) + pair[at].astype(F32)
            if ring is not None:
                value = value + ring[at].astype(F32)
            own[at] = value.astype(BF16)

    def send(self, i, step):
        self.ready(i, step)

        @when(step == 0)
        def _():
            for way in range(2):
                self.add(i, way, self.chunk(way, step), None)

        @when(step > 0)
        def _():
            for way in range(2):
                self.hop(i, way, step - 1).wait_recv()
                self.add(i, way, self.chunk(way, step), step)

        for way in range(2):
            self.hop(i, way, step).start()

    def finish(self, i, out):
        last = self.chips - 1
        for copy in self.exchange(i, self.z):
            copy.wait()
        for way in range(2):
            self.hop(i, way, last - 1).wait_recv()
            self.add(i, way, self.z, last)
        own = self.own(i, self.z)
        if i < 2:
            out[i] = own[...]
        else:
            bands, _, columns = own.shape
            for k in range(bands):
                out[i, :, columns * k : columns * (k + 1)] = own[k]

    def drain(self):
        for i in range(3):
            for way in range(2):

                @pl.loop(0, self.chips - 1)
                def _(step):
                    self.hop(i, way, step).wait_send()


def squares_of(ref):
    squares = jnp.zeros((8, 128), F32)
    for i in range(ref.shape[0]):
        value = ref[i].astype(F32)
        flat = jnp.sum((value * value).reshape(-1, 8, value.shape[1]), axis=0)
        for k in range(flat.shape[1] // 128):
            squares = squares + flat[:, 128 * k : 128 * (k + 1)]
    return squares


def weight_ring_kernel(n, *refs):
    a_ref, by_ref, mid_ref, by_both_ref, before_ref, out_ref, ss_ref, turned, parts, ss_send, ss_recv = refs[:11]
    ring = Ring(n, None, refs[11:])
    block, rest = mid_ref.shape[1], ring.chips - 1
    columns = ring.wide_own.shape[3] // block
    now = pl.program_id(0)
    me = ring.me

    @pl.when(now == 0)
    def _():
        ring.greet(True)
        parts[me] = squares_of(before_ref)
        turn(a_ref, by_ref, turned)

    @pl.when(now == columns)
    def _():
        ring.begin([2])

    @pl.when(now == 2 * columns)
    def _():
        ring.begin([0])

    @pl.when(now > columns)
    def _():
        ring.send(2, now - columns - 1)

    @pl.when(now > 2 * columns)
    def _():
        ring.send(0, now - 2 * columns - 1)

    @pl.when(now < columns)
    def _():
        value = rounded(turned[1], mid_ref[...]).T
        bands = block // ring.tall_own.shape[1]
        ring.tall_own[pl.ds(now * bands, bands)] = value.reshape(bands, -1, value.shape[1])

    @pl.when(now >= columns)
    def _():
        value = rounded(turned[0], by_both_ref[0]).reshape(n, -1, block)
        at = pl.ds(pl.multiple_of(lax.rem(now, columns) * block, block), block)
        ring.wide_own[now // columns - 1, :, :, at] = value

    @pl.when(now == 3 * columns - 1)
    def _():
        gate, down = columns - 1, 2 * columns - 1
        ring.begin([1])

        @pl.loop(0, rest)
        def _(step):
            @pl.when(gate + step < rest)
            def _():
                ring.send(0, gate + step)

            @pl.when(down + step < rest)
            def _():
                ring.send(2, down + step)

            ring.send(1, step)

        for i in (2, 0, 1):
            ring.finish(i, out_ref)
        parts[me] = parts[me] + squares_of(out_ref)
        ring.drain()

        def tell(k):
            return pltpu.make_async_remote_copy(
                src_ref=parts.at[me], dst_ref=parts.at[me], send_sem=ss_send.at[k], recv_sem=ss_recv.at[k],
                device_id={"dp": lax.rem(me + k, n)}, device_id_type=MESH,
            )

        for k in range(1, n):
            tell(k).start()
        for k in range(1, n):
            tell(k).wait()
        everyone = parts[0]
        for k in range(1, n):
            everyone = everyone + parts[k]
        ss_ref[...] = everyone


def shapes_of(n, d, ff):
    return (d // n, ff), (ff // d, d // n, d)


def weights_summed(n, a, by, mid, by_both, before, block=768):
    tokens, d = a.shape
    ff = mid.shape[1]
    wide, tall = shapes_of(n, d, ff)
    return pl.pallas_call(
        functools.partial(weight_ring_kernel, n),
        out_shape=(jax.ShapeDtypeStruct((3, *wide), BF16), jax.ShapeDtypeStruct((8, 128), F32)),
        grid=(3 * ff // block,),
        in_specs=[*part_specs(tokens, d, ff, block), pl.BlockSpec((3, *wide), lambda k: (0, 0, 0))],
        out_specs=(pl.BlockSpec((3, *wide), lambda k: (0, 0, 0)), pl.BlockSpec((8, 128), lambda k: (0, 0))),
        scratch_shapes=[
            pltpu.VMEM((2, d, tokens), BF16), pltpu.VMEM((n, 8, 128), F32), pltpu.SemaphoreType.DMA((n,)), pltpu.SemaphoreType.DMA((n,)),
            *Ring.scratch(n, wide, tall, True),
        ],
        compiler_params=params(63, collective_id=0, has_side_effects=True, dimension_semantics=("arbitrary",)),
        cost_estimate=cost(3, tokens, d, ff, 45 << 20),
        name="weights_summed",
    )(a, by, mid, by_both, before)


def first_kernel(n, block, *refs):
    wide_grads, tall_grads, w_gate, w_up, w_down, by_both1, h1, by1, a0 = refs[:9]
    out_ref, by_ref, by_both_ref, gate1, up1, gate0, up0, down0, fetched = refs[9:18]
    ring = Ring(n, [wide_grads.at[0], wide_grads.at[1], tall_grads], refs[18:])
    rest = ring.chips - 1
    tile = pl.program_id(0)
    moved = ((w_gate, 1, gate1), (w_up, 1, up1), (w_down, 0, down0), (w_gate, 0, gate0), (w_up, 0, up0))
    fetches = [pltpu.make_async_copy(w.at[number], to, fetched.at[k]) for k, (w, number, to) in enumerate(moved)]

    @pl.when(tile == 0)
    def _():
        for fetch in fetches:
            fetch.start()
        ring.greet(False)
        ring.begin([0, 1, 2])

    def have(*which):
        @pl.when(tile == 0)
        def _():
            for k in which:
                fetches[k].wait()

    def moment(which):
        step, i = 2 * tile + which // 3, which % 3

        @pl.when(step < rest)
        def _():
            ring.send(i, step)

        if which >= 3:

            @pl.when(step == rest)
            def _():
                ring.finish(i, out_ref)

    last = ((1,), (1,))
    have(0)
    by_gate_part = rounded(by_both1[0], gate1[...], last)
    moment(0)
    have(1)
    by_a = by_gate_part + rounded(by_both1[1], up1[...], last)
    wide, by_a = h1[...].astype(F32), by_a.astype(F32)
    scale = scale_of(wide)
    dots = jnp.sum(by_a * wide, -1, keepdims=True) / wide.shape[1]
    by_ref[...] = by1[...] + (by_a * scale - wide * (scale * scale * scale * dots)).astype(BF16)
    moment(1)
    have(2, 3, 4)

    @pl.loop(0, gate0.shape[1] // block)
    def _(k):
        at = pl.ds(pl.multiple_of(block * k, block), block)
        a = a0[...]
        by_mid = rounded(by_ref[...], down0[at, :], last)
        _, by_both_ref[0, :, at], by_both_ref[1, :, at] = gated_back(wide_dot(a, gate0[:, at]), wide_dot(a, up0[:, at]), by_mid)
        for part in range(3):

            @pl.when(k == part)
            def _():
                moment(2 + part)

    moment(5)

    @pl.when(tile == pl.num_programs(0) - 1)
    def _():
        ring.drain()


def first_layer(n, grads, by_both, h, by, a, w_gate, w_up, w_down, block=768):
    tokens, d = h.shape
    ff = by_both.shape[2]
    wide, tall = shapes_of(n, d, ff)
    deep = tokens // (n // 4)

    rows, both = pl.BlockSpec((deep, d), lambda i: (i, 0)), pl.BlockSpec((2, deep, ff), lambda i: (0, i, 0))
    return pl.pallas_call(
        functools.partial(first_kernel, n, block),
        out_shape=(
            jax.ShapeDtypeStruct((3, *wide), BF16),
            jax.ShapeDtypeStruct((tokens, d), BF16),
            jax.ShapeDtypeStruct((2, tokens, ff), BF16),
        ),
        grid=(n // 4,),
        in_specs=[EVERY] * 5 + [both, rows, rows, rows],
        out_specs=(pl.BlockSpec((3, *wide), lambda i: (0, 0, 0)), rows, both),
        scratch_shapes=[
            *(pltpu.VMEM(shape, BF16) for shape in ((d, ff), (d, ff), (d, ff), (d, ff), (ff, d))), pltpu.SemaphoreType.DMA((5,)),
            *Ring.scratch(n, wide, tall, False),
        ],
        compiler_params=params(63, collective_id=1, has_side_effects=True, dimension_semantics=("arbitrary",)),
        cost_estimate=cost(5, tokens, d, ff, 60 << 20),
        name="first_layer",
    )(
        grads[0].reshape(2, n // 2, 2, *wide), grads[1].reshape(n // 2, 2, *tall),
        w_gate, w_up, w_down, by_both, h, by, a,
    )


def adam_kernel(first, where_ref, factor_ref, *refs):
    pieces, (w, m, v) = refs[:4], (refs[4:7], refs[7:10], refs[10:13])
    new_w, new_m, new_v = (refs[i : i + 3] for i in ((13, 16, 19) if first else (22, 25, 28)))
    g_ref = refs[-1]
    part = pl.program_id(0)
    for p in range(4):

        @pl.when(part == p)
        def _():
            g_ref[...] = pieces[p][...]

    factor = factor_ref[0]
    for which in range(3):
        rows, columns = w[which].shape[1:]
        deep = g_ref.shape[1]
        for k in range(rows // deep):

            @pl.loop(0, deep // 16)
            def _(strip):
                at = (0, pl.ds(pl.multiple_of(deep * k + strip * 16, 16), 16), slice(None))
                g = g_ref[which, pl.ds(pl.multiple_of(strip * 16, 16), 16), columns * k : columns * (k + 1)].astype(F32) * factor
                mean = 0.9 * m[which][at] + 0.1 * g
                square = 0.95 * v[which][at] + 0.05 * g * g
                wide = w[which][at].astype(F32)
                new_m[which][at] = mean
                new_v[which][at] = square
                new_w[which][at] = (wide - 0.02 * (mean * lax.rsqrt(square + 1e-8) + 0.1 * wide)).astype(BF16)


def adam(n, where, factor, pieces, state, so_far):
    first = so_far is None
    shapes = [jax.ShapeDtypeStruct(s.shape, s.dtype) for s in state]

    def block(s):
        return pl.BlockSpec((1, s.shape[1] // n, s.shape[2]), lambda p, where, factor: (where[0, p], where[1, p], 0))

    whole = pl.BlockSpec(pieces[0].shape, lambda p, where, factor: (0, 0, 0))
    size = sum(s.size // n for s in state[:3]) * 4
    return pl.pallas_call(
        functools.partial(adam_kernel, first),
        out_shape=shapes,
        grid_spec=pltpu.PrefetchScalarGridSpec(
            num_scalar_prefetch=2,
            grid=(4,),
            in_specs=[whole] * 4 + [block(s) for s in state] + ([] if first else [EVERY] * 9),
            out_specs=[block(s) for s in state],
            scratch_shapes=[pltpu.VMEM(pieces[0].shape, BF16)],
        ),
        input_output_aliases={} if first else {15 + i: i for i in range(9)},
        compiler_params=params(48, dimension_semantics=("arbitrary",)),
        cost_estimate=pl.CostEstimate(flops=60_000_000, bytes_accessed=size * 11, transcendentals=size // 4),
        name="adam_step",
    )(where, factor, *pieces, *state, *(so_far or ()))


def solution(mesh):
    n = mesh.shape["dp"]
    chips = n // 2

    def step(x, dy, *arrays):
        weights, m, v = (arrays[i : i + 3] for i in (0, 3, 6))
        w_gate, w_up, w_down = weights
        x, dy = x[0], dy[0]
        a0, mid0 = forward_up(0, x, w_gate, w_up)
        h1 = forward_down(0, mid0, w_down, x)
        a1, all1 = last_layer(1, h1, dy, w_gate, w_up, w_down)
        grads1 = by_weights(a1, dy, all1)
        right, by, by_both0 = first_layer(n, grads1, all1, h1, dy, a0, w_gate, w_up, w_down)
        left, squares = weights_summed(n, a0, by, mid0, by_both0, right)
        count = sum(w.size for w in weights)
        factor = jnp.minimum(1.0, 0.5 * lax.rsqrt(jnp.sum(squares) / count + 1e-30)).reshape(1)

        me = lax.axis_index("dp")
        z, c = me // 2, me % 2
        ahead = [(i, (i + 2) % n) for i in range(n)]
        behind = [(i, (i + n - 2) % n) for i in range(n)]
        pairs = [(i, i ^ 1) for i in range(n)]
        new = None
        for hop in range(chips):
            if hop:
                right = lax.ppermute(right, "dp", ahead)
                left = lax.ppermute(left, "dp", behind)
            pieces = [right, lax.ppermute(right, "dp", pairs), left, lax.ppermute(left, "dp", pairs)]
            from_right, from_left = (z + chips - hop) % chips * 2, (z + hop) % chips * 2
            where = jnp.array([[1, 1, 0, 0], [0, 0, 0, 0]], jnp.int32).at[1].set(
                jnp.stack([from_right + c, from_right + 1 - c, from_left + c, from_left + 1 - c])
            )
            new = adam(n, where, factor, pieces, (*weights, *m, *v), new)
        return tuple(new)

    return jax.shard_map(
        step,
        mesh=mesh,
        in_specs=(P(("rep", "dp"), None, None),) * 2 + (P(None, None, None),) * 9,
        out_specs=(P("rep", None, None),) * 9,
        check_vma=False,
    )
```

```python
import functools

import jax
import jax.numpy as jnp
from jax import lax
from jax.experimental import pallas as pl
from jax.experimental.pallas import tpu as pltpu
from jax.sharding import PartitionSpec as P

MESH = pl.DeviceIdType.MESH
F32, BF16 = jnp.float32, jnp.bfloat16
EVERY = pl.BlockSpec(memory_space=pl.ANY)
VMEM = pl.BlockSpec(memory_space=pltpu.VMEM)


def rounded(a, b, contract=((1,), (0,))):
    return lax.dot_general(a, b, (contract, ((), ())), preferred_element_type=F32).astype(BF16)


def wide_dot(a, b):
    return jnp.dot(a, b, preferred_element_type=F32)


def scale_of(wide):
    return lax.rsqrt(jnp.mean(wide * wide, -1, keepdims=True) + 1e-6)


def normed(h):
    wide = h.astype(F32)
    return (wide * scale_of(wide)).astype(BF16)


def gated(gate, up):
    return (gate * jax.nn.sigmoid(gate) * up).astype(BF16)


def gated_back(gate, up, by_mid):
    by_mid = by_mid.astype(F32)
    one = jax.nn.sigmoid(gate)
    silu = gate * one
    by_gate = by_mid * up * (one * (1.0 + gate * (1.0 - one)))
    return (silu * up).astype(BF16), by_gate.astype(BF16), (by_mid * silu).astype(BF16)


def params(mib, **more):
    return pltpu.CompilerParams(vmem_limit_bytes=mib << 20, **more)


def cost(matmuls, tokens, d, ff, moved):
    return pl.CostEstimate(flops=2 * matmuls * tokens * d * ff, bytes_accessed=moved, transcendentals=tokens * ff)


def up_kernel(h_ref, gate_ref, up_ref, a_ref, mid_ref):
    @pl.when(pl.program_id(1) == 0)
    def _():
        a_ref[...] = normed(h_ref[...])

    a = a_ref[...]
    mid_ref[...] = gated(wide_dot(a, gate_ref[0]), wide_dot(a, up_ref[0]))


def columns_of(number, d, block):
    return pl.BlockSpec((1, d, block), lambda i, k: (number, 0, k))


def rows_of(number, d, block):
    return pl.BlockSpec((1, block, d), lambda i, k: (number, k, 0))


def forward_up(number, h, w_gate, w_up, tall=512, block=768):
    tokens, d = h.shape
    ff = w_gate.shape[2]
    rows = pl.BlockSpec((tall, d), lambda i, k: (i, 0))
    part = pl.BlockSpec((tall, block), lambda i, k: (i, k))
    return pl.pallas_call(
        up_kernel,
        out_shape=(jax.ShapeDtypeStruct((tokens, d), BF16), jax.ShapeDtypeStruct((tokens, ff), BF16)),
        grid=(tokens // tall, ff // block),
        in_specs=[rows, columns_of(number, d, block), columns_of(number, d, block)],
        out_specs=(rows, part),
        compiler_params=params(63),
        cost_estimate=cost(2, tokens, d, ff, 26 << 20),
        name="forward_up",
    )(h, w_gate, w_up)


def down_kernel(mid_ref, down_ref, h_ref, out_ref):
    out_ref[...] = h_ref[...] + rounded(mid_ref[...], down_ref[0])


def forward_down(number, mid, w_down, h, tall=512):
    tokens, d = h.shape
    ff = mid.shape[1]
    rows = pl.BlockSpec((tall, d), lambda i: (i, 0))
    return pl.pallas_call(
        down_kernel,
        out_shape=jax.ShapeDtypeStruct((tokens, d), BF16),
        grid=(tokens // tall,),
        in_specs=[pl.BlockSpec((tall, ff), lambda i: (i, 0)), pl.BlockSpec((1, ff, d), lambda i: (number, 0, 0)), rows],
        out_specs=rows,
        compiler_params=params(63),
        cost_estimate=cost(1, tokens, d, ff, 20 << 20),
        name="forward_down",
    )(mid, w_down, h)


def last_kernel(h_ref, by_ref, gate_ref, up_ref, down_ref, a_ref, all_ref):
    @pl.when(pl.program_id(1) == 0)
    def _():
        a_ref[...] = normed(h_ref[...])

    a = a_ref[...]
    by_mid = rounded(by_ref[...], down_ref[0], ((1,), (1,)))
    all_ref[2], all_ref[0], all_ref[1] = gated_back(wide_dot(a, gate_ref[0]), wide_dot(a, up_ref[0]), by_mid)


def last_layer(number, h, by, w_gate, w_up, w_down, tall=512, block=768):
    tokens, d = h.shape
    ff = w_gate.shape[2]
    rows = pl.BlockSpec((tall, d), lambda i, k: (i, 0))
    return pl.pallas_call(
        last_kernel,
        out_shape=(
            jax.ShapeDtypeStruct((tokens, d), BF16),
            jax.ShapeDtypeStruct((3, tokens, ff), BF16),
        ),
        grid=(tokens // tall, ff // block),
        in_specs=[rows, rows, columns_of(number, d, block), columns_of(number, d, block), rows_of(number, d, block)],
        out_specs=(rows, pl.BlockSpec((3, tall, block), lambda i, k: (0, i, k))),
        compiler_params=params(63),
        cost_estimate=cost(3, tokens, d, ff, 60 << 20),
        name="last_layer",
    )(h, by, w_gate, w_up, w_down)


def turn(a_ref, by_ref, turned):
    deep = 256

    @pl.loop(0, a_ref.shape[0] // deep)
    def _(k):
        at = pl.ds(pl.multiple_of(k * deep, deep), deep)
        turned[0, :, at] = a_ref[at, :].T
        turned[1, :, at] = by_ref[at, :].T


def part_specs(tokens, d, ff, block):
    count = ff // block
    whole = pl.BlockSpec((tokens, d), lambda k: (0, 0), pipeline_mode=pl.Buffered(1))
    mid = pl.BlockSpec((tokens, block), lambda k: (0, jnp.minimum(k, count - 1)))
    both = pl.BlockSpec((1, tokens, block), lambda k: (jnp.maximum(k - count, 0) // count, 0, jnp.maximum(k - count, 0) % count))
    return [whole, whole, mid, both]


def weight_kernel(a_ref, by_ref, all_ref, wide_ref, down_ref, turned):
    now = pl.program_id(0)
    tall = now < pl.num_programs(0) // 3

    @pl.when(now == 0)
    def _():
        turn(a_ref, by_ref, turned)

    value = rounded(turned[jnp.where(tall, 1, 0)], all_ref[0])

    @pl.when(tall)
    def _():
        down_ref[...] = value.T

    @pl.when(jnp.logical_not(tall))
    def _():
        wide_ref[0] = value


def by_weights(a, by, every, block=768):
    tokens, d = a.shape
    ff = every.shape[2]
    count = ff // block
    whole, _, _, both = part_specs(tokens, d, ff, block)
    stacked = pl.BlockSpec((1, tokens, block), lambda k: (jnp.where(k < count, 2, k // count - 1), 0, k % count))
    return pl.pallas_call(
        weight_kernel,
        out_shape=(jax.ShapeDtypeStruct((2, d, ff), BF16), jax.ShapeDtypeStruct((ff, d), BF16)),
        grid=(3 * count,),
        in_specs=[whole, whole, stacked],
        out_specs=(pl.BlockSpec((1, d, block), both.index_map), pl.BlockSpec((block, d), lambda k: (jnp.minimum(k, count - 1), 0))),
        scratch_shapes=[pltpu.VMEM((2, d, tokens), BF16)],
        compiler_params=params(63, dimension_semantics=("arbitrary",)),
        cost_estimate=cost(3, tokens, d, ff, 45 << 20),
        name="by_weights",
    )(a, by, every)


def when(condition):
    if isinstance(condition, bool):
        return (lambda body: body()) if condition else (lambda body: None)
    return pl.when(condition)


class Ring:
    def __init__(self, n, grads, refs):
        self.n, self.chips, self.grads = n, n // 2, grads
        self.wide_own, self.wide_pair, self.wide_ring, self.tall_own, self.tall_pair, self.tall_ring = refs[:6]
        self.local, self.pair_send, self.pair_recv, self.ring_send, self.ring_recv = refs[6:]
        self.me = lax.axis_index("dp")
        self.z, self.c = self.me // 2, lax.rem(self.me, 2)
        self.partner = self.z * 2 + 1 - self.c
        self.beside = [lax.rem(self.z + k, self.chips) * 2 + self.c for k in (1, self.chips - 1)]

    @staticmethod
    def scratch(n, wide, tall, all_own):
        chips, sem = n // 2, pltpu.SemaphoreType.DMA
        own = n if all_own else chips
        bands = tall[0]
        return [
            pltpu.VMEM((2, own, *wide), BF16),
            pltpu.VMEM((2, chips, *wide), BF16),
            pltpu.VMEM((2, chips - 1, *wide), BF16),
            pltpu.VMEM((own * bands, *tall[1:]), BF16),
            pltpu.VMEM((chips * bands, *tall[1:]), BF16),
            pltpu.VMEM(((chips - 1) * bands, *tall[1:]), BF16),
            sem((3, chips)), sem((3, chips)), sem((3, chips)), sem((3, 2, chips - 1)), sem((3, 2, chips - 1)),
        ]

    def chunk(self, way, step):
        return lax.rem(self.z + (self.chips - 1 - step if way == 0 else 1 + step), self.chips)

    def at(self, i, wide, tall, j):
        if i < 2:
            return wide.at[i, j]
        bands = self.tall_ring.shape[0] // (self.chips - 1)
        return tall.at[pl.ds(j * bands, bands)]

    def own(self, i, j, theirs=False):
        if self.grads is None:
            j = 2 * j + (1 - self.c if theirs else self.c)
        return self.at(i, self.wide_own, self.tall_own, j)

    def pair(self, i, j):
        return self.at(i, self.wide_pair, self.tall_pair, j)

    def arriving(self, i, step):
        return self.at(i, self.wide_ring, self.tall_ring, step)

    def exchange(self, i, j):
        theirs = self.own(i, j, True) if self.grads is None else self.grads[i].at[j, 1 - self.c]
        away = pltpu.make_async_remote_copy(
            src_ref=theirs, dst_ref=self.pair(i, j), send_sem=self.pair_send.at[i, j], recv_sem=self.pair_recv.at[i, j],
            device_id={"dp": self.partner}, device_id_type=MESH,
        )
        if self.grads is None:
            return [away]
        return [away, pltpu.make_async_copy(self.grads[i].at[j, self.c], self.own(i, j), self.local.at[i, j])]

    def greet(self, everyone):
        barrier = pltpu.get_barrier_semaphore()
        others = [lax.rem(self.me + k, self.n) for k in range(1, self.n)] if everyone else [self.partner, *self.beside]
        for other in others:
            pl.semaphore_signal(barrier, inc=1, device_id={"dp": other}, device_id_type=MESH)
        pl.semaphore_wait(barrier, len(others))

    def begin(self, matrices):
        half = self.chips // 2
        for step in range(half):
            for way in range(2 if step < half - 1 else 1):
                for i in matrices:
                    for copy in self.exchange(i, self.chunk(way, step)):
                        copy.start()
        for i in matrices:
            for copy in self.exchange(i, self.z):
                copy.start()

    def ready(self, i, step):
        half = self.chips // 2

        @when(step < half)
        def _():
            for copy in self.exchange(i, self.chunk(0, step)):
                copy.wait()

        @when(step < half - 1)
        def _():
            for copy in self.exchange(i, self.chunk(1, step)):
                copy.wait()

    def half(self, i, way):
        columns = self.pair(i, 0).shape[-1] // 2
        return (slice(None),) * (1 if i < 2 else 2) + (slice(columns * way, columns * (way + 1)),)

    def hop(self, i, way, step):
        at = self.half(i, way)
        return pltpu.make_async_remote_copy(
            src_ref=self.own(i, self.chunk(way, step)).at[at], dst_ref=self.arriving(i, step).at[at],
            send_sem=self.ring_send.at[i, way, step], recv_sem=self.ring_recv.at[i, way, step],
            device_id={"dp": self.beside[way]}, device_id_type=MESH,
        )

    def add(self, i, way, j, step):
        own, pair, columns = self.own(i, j), self.pair(i, j), self.half(i, way)[-1]
        ring = None if step is None else self.arriving(i, step - 1)

        @pl.loop(0, 3)
        def _(part):
            deep = own.shape[0] // 3
            at = (pl.ds(pl.multiple_of(part * deep, deep), deep), columns) if i < 2 else (pl.ds(part * deep, deep), slice(None), columns)
            value = own[at].astype(F32) + pair[at].astype(F32)
            if ring is not None:
                value = value + ring[at].astype(F32)
            own[at] = value.astype(BF16)

    def send(self, i, step):
        self.ready(i, step)

        @when(step == 0)
        def _():
            for way in range(2):
                self.add(i, way, self.chunk(way, step), None)

        @when(step > 0)
        def _():
            for way in range(2):
                self.hop(i, way, step - 1).wait_recv()
                self.add(i, way, self.chunk(way, step), step)

        for way in range(2):
            self.hop(i, way, step).start()

    def finish(self, i, out):
        last = self.chips - 1
        for copy in self.exchange(i, self.z):
            copy.wait()
        for way in range(2):
            self.hop(i, way, last - 1).wait_recv()
            self.add(i, way, self.z, last)
        own = self.own(i, self.z)
        if i < 2:
            out[i] = own[...]
        else:
            bands, _, columns = own.shape
            for k in range(bands):
                out[i, :, columns * k : columns * (k + 1)] = own[k]

    def drain(self):
        for i in range(3):
            for way in range(2):

                @pl.loop(0, self.chips - 1)
                def _(step):
                    self.hop(i, way, step).wait_send()


def squares_of(ref):
    def more(i, squares):
        value = ref[i].astype(F32)
        flat = jnp.sum((value * value).reshape(-1, 8, value.shape[1]), axis=0)
        for k in range(flat.shape[1] // 128):
            squares = squares + flat[:, 128 * k : 128 * (k + 1)]
        return squares

    return lax.fori_loop(0, ref.shape[0], more, jnp.zeros((8, 128), F32))


def weight_ring_kernel(n, *refs):
    a_ref, by_ref, mid_ref, by_both_ref, before_ref, out_ref, ss_ref, turned, parts, ss_send, ss_recv = refs[:11]
    ring = Ring(n, None, refs[11:])
    block, rest = mid_ref.shape[1], ring.chips - 1
    columns = ring.wide_own.shape[3] // block
    now = pl.program_id(0)
    me = ring.me

    @pl.when(now == 0)
    def _():
        ring.greet(True)
        parts[me] = squares_of(before_ref)
        turn(a_ref, by_ref, turned)

    @pl.when(now == columns)
    def _():
        ring.begin([2])

    @pl.when(now == 2 * columns)
    def _():
        ring.begin([0])

    @pl.when(now > columns)
    def _():
        ring.send(2, now - columns - 1)

    @pl.when(now > 2 * columns)
    def _():
        ring.send(0, now - 2 * columns - 1)

    @pl.when(now < columns)
    def _():
        value = rounded(turned[1], mid_ref[...]).T
        bands = block // ring.tall_own.shape[1]
        ring.tall_own[pl.ds(now * bands, bands)] = value.reshape(bands, -1, value.shape[1])

    @pl.when(now >= columns)
    def _():
        value = rounded(turned[0], by_both_ref[0]).reshape(n, -1, block)
        at = pl.ds(pl.multiple_of(lax.rem(now, columns) * block, block), block)
        ring.wide_own[now // columns - 1, :, :, at] = value

    @pl.when(now == 3 * columns - 1)
    def _():
        gate, down = columns - 1, 2 * columns - 1
        ring.begin([1])

        @pl.loop(0, rest)
        def _(step):
            @pl.when(gate + step < rest)
            def _():
                ring.send(0, gate + step)

            @pl.when(down + step < rest)
            def _():
                ring.send(2, down + step)

            ring.send(1, step)

        for i in (2, 0, 1):
            ring.finish(i, out_ref)
        parts[me] = parts[me] + squares_of(out_ref)
        ring.drain()

        def tell(k):
            return pltpu.make_async_remote_copy(
                src_ref=parts.at[me], dst_ref=parts.at[me], send_sem=ss_send.at[k], recv_sem=ss_recv.at[k],
                device_id={"dp": lax.rem(me + k, n)}, device_id_type=MESH,
            )

        for k in range(1, n):
            tell(k).start()
        for k in range(1, n):
            tell(k).wait()
        everyone = parts[0]
        for k in range(1, n):
            everyone = everyone + parts[k]
        ss_ref[...] = everyone


def shapes_of(n, d, ff):
    return (d // n, ff), (ff // d, d // n, d)


def weights_summed(n, a, by, mid, by_both, before, block=768):
    tokens, d = a.shape
    ff = mid.shape[1]
    wide, tall = shapes_of(n, d, ff)
    return pl.pallas_call(
        functools.partial(weight_ring_kernel, n),
        out_shape=(jax.ShapeDtypeStruct((3, *wide), BF16), jax.ShapeDtypeStruct((8, 128), F32)),
        grid=(3 * ff // block,),
        in_specs=[*part_specs(tokens, d, ff, block), pl.BlockSpec((3, *wide), lambda k: (0, 0, 0))],
        out_specs=(pl.BlockSpec((3, *wide), lambda k: (0, 0, 0)), pl.BlockSpec((8, 128), lambda k: (0, 0))),
        scratch_shapes=[
            pltpu.VMEM((2, d, tokens), BF16), pltpu.VMEM((n, 8, 128), F32), pltpu.SemaphoreType.DMA((n,)), pltpu.SemaphoreType.DMA((n,)),
            *Ring.scratch(n, wide, tall, True),
        ],
        compiler_params=params(63, collective_id=0, has_side_effects=True, dimension_semantics=("arbitrary",)),
        cost_estimate=cost(3, tokens, d, ff, 45 << 20),
        name="weights_summed",
    )(a, by, mid, by_both, before)


def first_kernel(n, block, *refs):
    wide_grads, tall_grads, w_gate, w_up, w_down, by_both1, h1, by1, a0 = refs[:9]
    out_ref, by_ref, by_both_ref, gate1, up1, gate0, up0, down0, fetched = refs[9:18]
    ring = Ring(n, [wide_grads.at[0], wide_grads.at[1], tall_grads], refs[18:])
    rest = ring.chips - 1
    tile = pl.program_id(0)
    moved = ((w_gate, 1, gate1), (w_up, 1, up1), (w_down, 0, down0), (w_gate, 0, gate0), (w_up, 0, up0))
    fetches = [pltpu.make_async_copy(w.at[number], to, fetched.at[k]) for k, (w, number, to) in enumerate(moved)]

    @pl.when(tile == 0)
    def _():
        for fetch in fetches:
            fetch.start()
        ring.greet(False)
        ring.begin([0, 1, 2])

    def have(*which):
        @pl.when(tile == 0)
        def _():
            for k in which:
                fetches[k].wait()

    def moment(which):
        step, i = 2 * tile + which // 3, which % 3

        @pl.when(step < rest)
        def _():
            ring.send(i, step)

        if which >= 3:

            @pl.when(step == rest)
            def _():
                ring.finish(i, out_ref)

    last = ((1,), (1,))
    have(0)
    by_gate_part = rounded(by_both1[0], gate1[...], last)
    moment(0)
    have(1)
    by_a = by_gate_part + rounded(by_both1[1], up1[...], last)
    wide, by_a = h1[...].astype(F32), by_a.astype(F32)
    scale = scale_of(wide)
    dots = jnp.sum(by_a * wide, -1, keepdims=True) / wide.shape[1]
    by_ref[...] = by1[...] + (by_a * scale - wide * (scale * scale * scale * dots)).astype(BF16)
    moment(1)
    have(2, 3, 4)

    @pl.loop(0, gate0.shape[1] // block)
    def _(k):
        at = pl.ds(pl.multiple_of(block * k, block), block)
        a = a0[...]
        by_mid = rounded(by_ref[...], down0[at, :], last)
        _, by_both_ref[0, :, at], by_both_ref[1, :, at] = gated_back(wide_dot(a, gate0[:, at]), wide_dot(a, up0[:, at]), by_mid)
        for part in range(3):

            @pl.when(k == part)
            def _():
                moment(2 + part)

    moment(5)

    @pl.when(tile == pl.num_programs(0) - 1)
    def _():
        ring.drain()


def first_layer(n, grads, by_both, h, by, a, w_gate, w_up, w_down, block=768):
    tokens, d = h.shape
    ff = by_both.shape[2]
    wide, tall = shapes_of(n, d, ff)
    deep = tokens // (n // 4)

    rows, both = pl.BlockSpec((deep, d), lambda i: (i, 0)), pl.BlockSpec((2, deep, ff), lambda i: (0, i, 0))
    return pl.pallas_call(
        functools.partial(first_kernel, n, block),
        out_shape=(
            jax.ShapeDtypeStruct((3, *wide), BF16),
            jax.ShapeDtypeStruct((tokens, d), BF16),
            jax.ShapeDtypeStruct((2, tokens, ff), BF16),
        ),
        grid=(n // 4,),
        in_specs=[EVERY] * 5 + [both, rows, rows, rows],
        out_specs=(pl.BlockSpec((3, *wide), lambda i: (0, 0, 0)), rows, both),
        scratch_shapes=[
            *(pltpu.VMEM(shape, BF16) for shape in ((d, ff), (d, ff), (d, ff), (d, ff), (ff, d))), pltpu.SemaphoreType.DMA((5,)),
            *Ring.scratch(n, wide, tall, False),
        ],
        compiler_params=params(63, collective_id=1, has_side_effects=True, dimension_semantics=("arbitrary",)),
        cost_estimate=cost(5, tokens, d, ff, 60 << 20),
        name="first_layer",
    )(
        grads[0].reshape(2, n // 2, 2, *wide), grads[1].reshape(n // 2, 2, *tall),
        w_gate, w_up, w_down, by_both, h, by, a,
    )


def adam_kernel(first, where_ref, factor_ref, *refs):
    pieces, (w, m, v) = refs[:4], (refs[4:7], refs[7:10], refs[10:13])
    new_w, new_m, new_v = (refs[i : i + 3] for i in ((13, 16, 19) if first else (22, 25, 28)))
    g_ref = refs[-1]
    part = pl.program_id(0)
    for p in range(4):

        @pl.when(part == p)
        def _():
            @pl.loop(0, g_ref.shape[0])
            def _(k):
                g_ref[k] = pieces[p][k]

    factor = factor_ref[0]
    for which in range(3):
        rows, columns = w[which].shape[1:]
        deep = g_ref.shape[1]
        for k in range(rows // deep):

            @pl.loop(0, deep // 16)
            def _(strip):
                at = (0, pl.ds(pl.multiple_of(deep * k + strip * 16, 16), 16), slice(None))
                g = g_ref[which, pl.ds(pl.multiple_of(strip * 16, 16), 16), columns * k : columns * (k + 1)].astype(F32) * factor
                mean = 0.9 * m[which][at] + 0.1 * g
                square = 0.95 * v[which][at] + 0.05 * g * g
                wide = w[which][at].astype(F32)
                new_m[which][at] = mean
                new_v[which][at] = square
                new_w[which][at] = (wide - 0.02 * (mean * lax.rsqrt(square + 1e-8) + 0.1 * wide)).astype(BF16)


def adam(n, where, factor, pieces, state, so_far):
    first = so_far is None
    shapes = [jax.ShapeDtypeStruct(s.shape, s.dtype) for s in state]

    def block(s):
        return pl.BlockSpec((1, s.shape[1] // n, s.shape[2]), lambda p, where, factor: (where[0, p], where[1, p], 0))

    whole = pl.BlockSpec(pieces[0].shape, lambda p, where, factor: (0, 0, 0))
    size = sum(s.size // n for s in state[:3]) * 4
    return pl.pallas_call(
        functools.partial(adam_kernel, first),
        out_shape=shapes,
        grid_spec=pltpu.PrefetchScalarGridSpec(
            num_scalar_prefetch=2,
            grid=(4,),
            in_specs=[whole] * 4 + [block(s) for s in state] + ([] if first else [EVERY] * 9),
            out_specs=[block(s) for s in state],
            scratch_shapes=[pltpu.VMEM(pieces[0].shape, BF16)],
        ),
        input_output_aliases={} if first else {15 + i: i for i in range(9)},
        compiler_params=params(48, dimension_semantics=("arbitrary",)),
        cost_estimate=pl.CostEstimate(flops=60_000_000, bytes_accessed=size * 11, transcendentals=size // 4),
        name="adam_step",
    )(where, factor, *pieces, *state, *(so_far or ()))


def solution(mesh):
    n = mesh.shape["dp"]
    chips = n // 2

    def step(x, dy, *arrays):
        weights, m, v = (arrays[i : i + 3] for i in (0, 3, 6))
        w_gate, w_up, w_down = weights
        x, dy = x[0], dy[0]
        a0, mid0 = forward_up(0, x, w_gate, w_up)
        h1 = forward_down(0, mid0, w_down, x)
        a1, all1 = last_layer(1, h1, dy, w_gate, w_up, w_down)
        grads1 = by_weights(a1, dy, all1)
        right, by, by_both0 = first_layer(n, grads1, all1, h1, dy, a0, w_gate, w_up, w_down)
        left, squares = weights_summed(n, a0, by, mid0, by_both0, right)
        count = sum(w.size for w in weights)
        factor = jnp.minimum(1.0, 0.5 * lax.rsqrt(jnp.sum(squares) / count + 1e-30)).reshape(1)

        me = lax.axis_index("dp")
        z, c = me // 2, me % 2
        ahead = [(i, (i + 2) % n) for i in range(n)]
        behind = [(i, (i + n - 2) % n) for i in range(n)]
        pairs = [(i, i ^ 1) for i in range(n)]
        new = None
        for hop in range(chips):
            if hop:
                right = lax.ppermute(right, "dp", ahead)
                left = lax.ppermute(left, "dp", behind)
            pieces = [right, lax.ppermute(right, "dp", pairs), left, lax.ppermute(left, "dp", pairs)]
            from_right, from_left = (z + chips - hop) % chips * 2, (z + hop) % chips * 2
            where = jnp.array([[1, 1, 0, 0], [0, 0, 0, 0]], jnp.int32).at[1].set(
                jnp.stack([from_right + c, from_right + 1 - c, from_left + c, from_left + 1 - c])
            )
            new = adam(n, where, factor, pieces, (*weights, *m, *v), new)
        return tuple(new)

    return jax.shard_map(
        step,
        mesh=mesh,
        in_specs=(P(("rep", "dp"), None, None),) * 2 + (P(None, None, None),) * 9,
        out_specs=(P("rep", None, None),) * 9,
        check_vma=False,
    )
```
